32 devices in a mesh: feat: 4 (over y, core), dom: 8 (over z, x).
Axes of the slice: x: 2, y: 2, z: 4, core: 2. Of those that a mesh axis runs over, the one named last changes fastest.
Arguments:
- features: bfloat16 [32768, 128], P('dom'), may hold values from -6 to 6
- w_input: bfloat16 [128, 256], P(None, 'feat'), may hold values from -0.5 to 0.5
- layer_weights: bfloat16 [4, 256, 256], replicated, may hold values from -0.375 to 0.375
- history: bfloat16 [4, 32768, 256], P(None, 'dom', 'feat'), may hold values from 0 to 2
- tile_values: bfloat16 [256, 6, 128, 128], P('dom'), may hold values from -0.21875 to 0.21875
- tile_columns: int32 [256, 6], P('dom'), may hold values from 0 to 63, as said below
- send_rows: int32 [8, 8, 512], P('dom'), may hold values from 0 to 4095
- send_counts: int32 [8, 8], P('dom'), may hold values from 0 to 512, as said below
Outputs:
- pushed: bfloat16 [4, 32768, 256], P(None, 'dom', 'feat')
- final_rows: bfloat16 [32768, 256], P('dom', 'feat')
The draws below stay inside these ranges and needn't reach their ends.
Inputs may be any that keep to these rules, and one draw needn't show every extreme that they name: `tile_columns`: per row of tiles the first 2 entries lie below 4096 / 128 (own rows), the others at or above it (halo slots); every halo column tile of every partition is named somewhere. `send_counts`: A partition sends nothing to itself; in every draw some destination receives exactly 512 rows from every other partition.
All inputs are finite; a program needn't handle non-finite values.
Results may differ from the reference program's by a relative error of at most 0.0052.
Values may be sent and summed in bfloat16 or wider, within the bound.
No kernel may reach another device: no remote copies, remote signals or barrier semaphores. Data moves between devices by JAX's collectives and lax.ppermute only.
A program may use at most 128 MiB of HBM per device.

```python
import math
import jax
import jax.numpy as jnp
from jax import lax

F = 256
IN_FEAT = 128
NODES_DEV = 4096
CAP = 512
TILE = 128
K = 6
K_LOC = 2
LAYERS = 4
NODES = 32768
HALO = 4096
ROW_TILES = 256
N_DOM = 8


def shuffle_one(sub_key, span):
    return jax.random.permutation(sub_key, span)


def draw_tile_columns(key, part):
    local_tiles = NODES_DEV // TILE
    halo_tiles = HALO // TILE
    remote_count = K - K_LOC
    key_local, key_shuffle = jax.random.split(key)
    local_cols = jax.random.randint(key_local, (ROW_TILES, K_LOC), 0, local_tiles)
    block_keys = jax.random.split(key_shuffle, N_DOM)
    span = local_tiles * remote_count
    shuffled = jax.vmap(lambda sub_key: shuffle_one(sub_key, span))(block_keys)
    remote = local_tiles + shuffled % halo_tiles
    remote = remote.reshape(ROW_TILES, remote_count)
    return jnp.concatenate([local_cols, remote], axis=1).astype(jnp.int32)


def draw_send_counts(key, part):
    key_heavy, key_high, key_low, key_busy = jax.random.split(key, 4)
    dest_ids = jnp.arange(N_DOM)
    busiest = jax.random.randint(key_busy, (), 0, N_DOM)
    heavy_dest = (jax.random.randint(key_heavy, (N_DOM,), 0, 4) == 0) | (dest_ids == busiest)
    high_counts = jax.random.randint(key_high, (N_DOM, N_DOM), CAP // 2, CAP + 1)
    low_counts = jax.random.randint(key_low, (N_DOM, N_DOM), (CAP + 7) // 8, CAP // 2 + 1)
    counts = jnp.where(heavy_dest[None, :], high_counts, low_counts)
    counts = jnp.where(dest_ids[None, :] == busiest, CAP, counts)
    counts = jnp.where(dest_ids[:, None] == dest_ids[None, :], 0, counts)
    return counts.astype(jnp.int32)


def touch_ends(drawn, rng, low, top_value):
    place = [jax.random.randint(jax.random.fold_in(rng, axis), (), 0, length) for axis, length in enumerate(drawn.shape)]
    main_axis = drawn.shape.index(max(drawn.shape))
    neighbour = place[:main_axis] + [(place[main_axis] + 1) % drawn.shape[main_axis]] + place[main_axis + 1:]
    return drawn.at[tuple(place)].set(low).at[tuple(neighbour)].set(top_value)


def shard_levels(rng, extent, shards, least, largest):
    gain = 1.0
    for dim, parts in shards:
        draws = jax.random.uniform(jax.random.fold_in(jax.random.fold_in(rng, 6), dim), (parts,), jnp.float32, least / len(shards), largest / len(shards))
        gain = gain * jnp.repeat(jnp.exp(draws), extent[dim] // parts).reshape((-1,) + (1,) * (len(extent) - 1 - dim))
    return gain


def normal_values(key, dims, spread, reach, pieces=(), kind=jnp.bfloat16):
    drawn = jax.random.normal(key, dims, jnp.float32) * spread
    if len(pieces) > 0:
        drawn = shard_levels(key, dims, pieces, -0.22, 0.18) * drawn
    return jnp.clip(drawn, min=-reach, max=reach).astype(kind)


def setup_inputs(seed: int = 0) -> dict:
    splits = jax.random.split(jax.random.key(seed), 9)
    features = normal_values(splits[0], (NODES, IN_FEAT), 1.0, 6.0, ((0, 8),))
    w_input = normal_values(splits[1], (IN_FEAT, F), IN_FEAT ** -0.5, 0.5, ((1, 4),))
    layer_weights = normal_values(splits[2], (LAYERS, F, F), F ** -0.5, 0.375)
    history = jnp.clip(2.0 * jax.random.uniform(splits[3], (LAYERS, NODES, F), jnp.float32) ** shard_levels(splits[3], (LAYERS, NODES, F), ((1, 8), (2, 4)), -0.2, 0.2), 0.0, 2.0).astype(jnp.bfloat16)
    tile_values = normal_values(splits[4], (ROW_TILES, K, TILE, TILE), (K * TILE) ** -0.5, 0.21875, ((0, 8),))
    tile_columns = draw_tile_columns(jax.random.fold_in(splits[8], 71), 0)
    send_rows = touch_ends(jax.random.randint(splits[6], (N_DOM, N_DOM, CAP), 0, NODES_DEV), jax.random.fold_in(splits[6], 1), 0, NODES_DEV - 1).astype(jnp.int32)
    send_counts = draw_send_counts(jax.random.fold_in(splits[8], 71), 0)
    return dict(features=features, w_input=w_input, layer_weights=layer_weights, history=history, tile_values=tile_values, tile_columns=tile_columns, send_rows=send_rows, send_counts=send_counts)


ALPHA = 0.1
LAMBDA_DECAY = 0.5


def reference(features, w_input, layer_weights, history, tile_values, tile_columns, send_rows, send_counts):
    initial = jnp.maximum(jnp.dot(features, w_input, preferred_element_type=jnp.float32), 0.0).astype(jnp.bfloat16)
    slot_ids = jnp.arange(CAP)
    sources = jnp.arange(N_DOM)
    local_tiles = NODES_DEV // TILE
    pushed = []
    current = initial
    for layer_index in range(LAYERS):
        beta_layer = math.log(LAMBDA_DECAY / (layer_index + 1) + 1.0)
        layer_table = history[layer_index]

        def one_part(part_index):
            source_rows = sources[:, None] * NODES_DEV + send_rows[:, part_index, :]
            live_mask = slot_ids[None, :] < send_counts[:, part_index][:, None]
            halo_rows = jnp.where(live_mask[:, :, None], layer_table[source_rows], jnp.zeros((), jnp.bfloat16))
            halo_rows = halo_rows.reshape(N_DOM * CAP, F)
            own_rows = lax.dynamic_slice_in_dim(current, (part_index * NODES_DEV).astype(jnp.int32), NODES_DEV, 0)
            combined = jnp.concatenate([own_rows, halo_rows], axis=0).reshape(-1, TILE, F)
            columns = lax.dynamic_slice_in_dim(tile_columns, (part_index * local_tiles).astype(jnp.int32), local_tiles, 0)
            values = lax.dynamic_slice_in_dim(tile_values, (part_index * local_tiles).astype(jnp.int32), local_tiles, 0)
            picked = combined[columns]
            summed = jnp.einsum('rkab,rkbf->raf', values.astype(jnp.float32), picked.astype(jnp.float32))
            return summed.reshape(NODES_DEV, F)

        aggregated = lax.map(one_part, jnp.arange(N_DOM, dtype=jnp.int32)).reshape(NODES, F)
        blended = ((1.0 - ALPHA) * aggregated + ALPHA * initial.astype(jnp.float32)).astype(jnp.bfloat16)
        blended = lax.optimization_barrier(blended)
        product = jnp.dot(blended, layer_weights[layer_index], preferred_element_type=jnp.float32)
        fresh = jnp.maximum((1.0 - beta_layer) * blended.astype(jnp.float32) + beta_layer * product, 0.0)
        pushed.append(current)
        current = fresh.astype(jnp.bfloat16)
    return jnp.stack(pushed), current
```

```python
import functools
import math

import jax
import jax.numpy as jnp
from jax import lax
from jax.experimental import pallas as pl
from jax.experimental.pallas import tpu as pltpu
from jax.sharding import PartitionSpec as P

ALPHA = 0.1
LAMBDA_DECAY = 0.5
OWN_TILES_PER_ROW = 2
LANES = 128
NT = (((1,), (1,)), ((), ()))
F32 = jnp.float32
BF16 = jnp.bfloat16


def gather_kernel(me_ref, rows_ref, counts_ref, hist_ref, *refs):
    layers, width, nodes = hist_ref.shape
    outs, scratch = refs[:layers], refs[layers:]
    groups = len(scratch) // 2
    tables, picked = scratch[:groups], scratch[groups:]
    per_group = layers // groups
    dest = pl.program_id(0) ^ me_ref[0]
    slots = picked[0].shape[0]

    @pl.when(pl.program_id(0) == 0)
    def _():
        for g in range(groups):
            for start in range(0, nodes, 512):
                part = hist_ref[g * per_group : (g + 1) * per_group, :, start : start + 512]
                part = part.reshape(per_group * width, 512).astype(F32)
                tables[g][start : start + 512, :] = part.T

    def step(block, carry):
        base = pl.multiple_of(block * 16, 16)
        for u in range(16):
            row = rows_ref[dest, base + u]
            for g in range(groups):
                picked[g][pl.ds(base + u, 1), :] = tables[g][pl.ds(row, 1), :]
        return carry

    lax.fori_loop(0, slots // 16, step, 0)
    live = lax.broadcasted_iota(jnp.int32, (1, slots), 1) < counts_ref[0, dest]
    for g in range(groups):
        turned = jnp.where(live, picked[g][...].T, 0.0).astype(BF16)
        for i in range(per_group):
            outs[g * per_group + i][0] = turned[i * width : (i + 1) * width, :]


def gather_halo(me, send_rows, send_counts, hist):
    layers, width, nodes = hist.shape
    peers, slots = send_rows.shape
    groups = layers * width // LANES
    by_dest = pl.BlockSpec((1, width, slots), lambda k, me, rows, counts: (k ^ me[0], 0, 0))
    by_shift = pl.BlockSpec((1, width, slots), lambda k, me, rows, counts: (k, 0, 0))
    return pl.pallas_call(
        gather_kernel,
        grid_spec=pltpu.PrefetchScalarGridSpec(
            num_scalar_prefetch=3,
            grid=(peers,),
            in_specs=[pl.BlockSpec(hist.shape, lambda k, me, rows, counts: (0, 0, 0))],
            out_specs=[by_dest] + [by_shift] * (layers - 1),
            scratch_shapes=[pltpu.VMEM((nodes, LANES), F32)] * groups
            + [pltpu.VMEM((slots, LANES), F32)] * groups,
        ),
        out_shape=[jax.ShapeDtypeStruct((peers, width, slots), BF16)] * layers,
        name="gather_halo",
    )(me, send_rows, send_counts, hist)


def tiles_dot(left_tiles, values):
    left = jnp.concatenate(left_tiles, axis=1)
    right = jnp.concatenate([values[k] for k in range(values.shape[0])], axis=1)
    return lax.dot_general(left, right, NT, preferred_element_type=F32)


def own_share(cols_ref, values_ref, state, first_row, row, tile):
    picks = []
    for k in range(OWN_TILES_PER_ROW):
        start = pl.multiple_of(cols_ref[first_row + row, k] * tile, tile)
        picks.append(state[:, pl.ds(start, tile)])
    return tiles_dot(picks, values_ref[row])


def blend(agg, initial):
    return ((1.0 - ALPHA) * agg + ALPHA * initial.astype(F32)).astype(BF16)


def first_kernel(steps, cols_ref, feat_ref, w_ref, values_ref, h_ref, loc_ref, state):
    i = pl.program_id(0)
    rows, _, tile, _ = values_ref.shape
    span = rows * tile

    @pl.when(i == 0)
    def _():
        prod = lax.dot_general(w_ref[...], feat_ref[...], NT, preferred_element_type=F32)
        h0 = jnp.maximum(prod, 0.0).astype(BF16)
        state[...] = h0
        h_ref[...] = h0

    for r in range(rows):
        loc_ref[:, r * tile : (r + 1) * tile] = own_share(
            cols_ref, values_ref, state, i * rows, r, tile
        )


def first_call(cols, features, w_t, values, steps):
    nodes = features.shape[0]
    width = w_t.shape[0]
    row_tiles, per_row, tile, _ = values.shape
    rows = row_tiles // steps
    whole = lambda shape: pl.BlockSpec(shape, lambda i, c: (0,) * len(shape))
    return pl.pallas_call(
        functools.partial(first_kernel, steps),
        grid_spec=pltpu.PrefetchScalarGridSpec(
            num_scalar_prefetch=1,
            grid=(steps,),
            in_specs=[
                whole(features.shape),
                whole(w_t.shape),
                pl.BlockSpec((rows, OWN_TILES_PER_ROW, tile, tile), lambda i, c: (i, 0, 0, 0)),
            ],
            out_specs=[
                whole((width, nodes)),
                pl.BlockSpec((width, rows * tile), lambda i, c: (0, i)),
            ],
            scratch_shapes=[pltpu.VMEM((width, nodes), BF16)],
        ),
        out_shape=[
            jax.ShapeDtypeStruct((width, nodes), BF16),
            jax.ShapeDtypeStruct((width, nodes), F32),
        ],
        name="first_own",
    )(cols, features, w_t, values)


def halo_kernel(pieces, blended, own_tiles, cols_ref, *refs):
    i = pl.program_id(0)
    halo_refs = refs[:pieces]
    refs = refs[pieces:]
    n_values = len(refs) - (3 if blended else 1) - (1 if pieces > 1 else 0)
    values_refs, refs = refs[:n_values], refs[n_values:]
    rows, _, tile, _ = values_refs[0].shape
    if pieces > 1:
        halo = refs[-1]

        @pl.when(i == 0)
        def _():
            halo[0] = jnp.zeros(halo.shape[1:], BF16)
            for k in range(pieces):
                halo[k + 1] = halo_refs[k][...]

    else:
        halo = halo_refs[0]
    out_ref = refs[2] if blended else refs[0]
    per_peer = halo.shape[2] // tile
    for r in range(rows):
        picks = []
        for k in range(OWN_TILES_PER_ROW, OWN_TILES_PER_ROW * (1 + n_values)):
            slot = cols_ref[i * rows + r, k] - own_tiles
            start = pl.multiple_of((slot % per_peer) * tile, tile)
            picks.append(halo[slot // per_peer, :, pl.ds(start, tile)])
        values = jnp.concatenate([v[r] for v in values_refs], axis=0)
        agg = tiles_dot(picks, values)
        at = slice(r * tile, (r + 1) * tile)
        if blended:
            out_ref[:, at] = blend(refs[0][:, at] + agg, refs[1][:, at])
        else:
            out_ref[:, at] = agg


def halo_call(cols, halos, values, own_tiles, steps, peers, extra=()):
    row_tiles, per_row, tile, _ = values.shape
    rows = row_tiles // steps
    width, slots = halos[0].shape[-2:]
    n_values = per_row // OWN_TILES_PER_ROW - 1
    whole = lambda shape: pl.BlockSpec(shape, lambda i, c: (0,) * len(shape))
    column = pl.BlockSpec((width, rows * tile), lambda i, c: (0, i))
    values_spec = lambda n: pl.BlockSpec(
        (rows, OWN_TILES_PER_ROW, tile, tile), lambda i, c: (i, n, 0, 0)
    )
    scratch = [pltpu.VMEM((peers, width, slots), BF16)] if len(halos) > 1 else []
    return pl.pallas_call(
        functools.partial(halo_kernel, len(halos), bool(extra), own_tiles),
        grid_spec=pltpu.PrefetchScalarGridSpec(
            num_scalar_prefetch=1,
            grid=(steps,),
            in_specs=[whole(h.shape) for h in halos]
            + [values_spec(n + 1) for n in range(n_values)]
            + [column for _ in extra],
            out_specs=column,
            scratch_shapes=scratch,
        ),
        out_shape=jax.ShapeDtypeStruct((width, row_tiles * tile), BF16 if extra else F32),
        name="halo_share",
    )(cols, *halos, *([values] * n_values), *extra)


def fresh_rows(beta, weight, parts):
    joined = jnp.concatenate(parts, axis=0)
    product = jnp.dot(weight, joined, preferred_element_type=F32)
    return jnp.maximum((1.0 - beta) * parts[0].astype(F32) + beta * product, 0.0).astype(BF16)


def step_kernel(beta, pieces, front, cols_ref, *refs):
    parts = refs[:pieces]
    w_ref, values_ref, halo_ref, h0_ref, h_ref, z_ref, state = refs[pieces:]
    i = pl.program_id(0)
    rows, _, tile, _ = values_ref.shape

    @pl.when(i < front)
    def _():
        fresh = fresh_rows(beta, w_ref[...], [p[...] for p in parts])
        span = fresh.shape[1]
        h_ref[...] = fresh
        state[:, pl.ds(pl.multiple_of(i * span, span), span)] = fresh

    @pl.when(i >= front)
    def _():
        for r in range(rows):
            agg = own_share(cols_ref, values_ref, state, (i - front) * rows, r, tile)
            at = slice(r * tile, (r + 1) * tile)
            z_ref[:, at] = blend(agg + halo_ref[:, at], h0_ref[:, at])


def step_call(beta, cols, parts, weight, values, halo_agg, h0, front, back):
    width, nodes = h0.shape
    row_tiles, per_row, tile, _ = values.shape
    rows = row_tiles // back
    early = lambda i, c: (0, jnp.minimum(i, front - 1))
    late = lambda i, c: (0, jnp.maximum(i - front, 0))
    late_block = pl.BlockSpec((width, rows * tile), late)
    return pl.pallas_call(
        functools.partial(step_kernel, beta, len(parts), front),
        grid_spec=pltpu.PrefetchScalarGridSpec(
            num_scalar_prefetch=1,
            grid=(front + back,),
            in_specs=[pl.BlockSpec((width, nodes // front), early) for _ in parts]
            + [
                pl.BlockSpec(weight.shape, lambda i, c: (0, 0)),
                pl.BlockSpec(
                    (rows, OWN_TILES_PER_ROW, tile, tile),
                    lambda i, c: (jnp.maximum(i - front, 0), 0, 0, 0),
                ),
                late_block,
                late_block,
            ],
            out_specs=[pl.BlockSpec((width, nodes // front), early), late_block],
            scratch_shapes=[pltpu.VMEM((width, nodes), BF16)],
        ),
        out_shape=[jax.ShapeDtypeStruct((width, nodes), BF16)] * 2,
        name="layer_step",
    )(cols, *parts, weight, values, halo_agg, h0)


def last_kernel(beta, *refs):
    *parts, w_ref, h_ref = refs
    h_ref[...] = fresh_rows(beta, w_ref[...], [p[...] for p in parts])


def last_call(beta, parts, weight, steps):
    width, nodes = parts[0].shape
    column = pl.BlockSpec((width, nodes // steps), lambda i: (0, i))
    return pl.pallas_call(
        functools.partial(last_kernel, beta),
        grid=(steps,),
        in_specs=[column] * len(parts) + [pl.BlockSpec(weight.shape, lambda i: (0, 0))],
        out_specs=column,
        out_shape=jax.ShapeDtypeStruct((width, nodes), BF16),
        name="last_step",
    )(*parts, weight)


def flip(array, axis, size, shift):
    return lax.ppermute(array, axis, [(i, i ^ shift) for i in range(size)])


def feat_parts(z, n_feat):
    parts = [None] * n_feat
    parts[0] = z
    for shift in range(2, n_feat, 2):
        parts[shift] = flip(z, "feat", n_feat, shift)
    for shift in range(0, n_feat, 2):
        parts[shift + 1] = flip(parts[shift], "feat", n_feat, 1)
    return parts


def on_device(
    n_feat, n_dom, features, w_input, layer_weights, history, tile_values, tile_columns,
    send_rows, send_counts,
):
    layers = history.shape[0]
    nodes = features.shape[0]
    width = w_input.shape[1]
    tile = tile_values.shape[-1]
    own_tiles = nodes // tile
    slots = send_rows.shape[2]
    me = lax.axis_index("dom")
    feat = lax.axis_index("feat")
    steps = 4

    sends = gather_halo(
        me[None], send_rows[0], send_counts, jnp.swapaxes(history, 1, 2)
    )
    per_peer = slots // tile
    slot = tile_columns - own_tiles
    by_shift = own_tiles + ((slot // per_peer) ^ me) * per_peer + slot % per_peer
    shift_columns = jnp.where(tile_columns < own_tiles, tile_columns, by_shift)

    mine = lax.dynamic_slice_in_dim(layer_weights, feat * width, width, 2)
    weights = jnp.concatenate(
        [
            lax.dynamic_slice_in_dim(mine, (feat ^ shift) * width, width, 1)
            for shift in range(n_feat)
        ],
        axis=1,
    )
    weights = jnp.swapaxes(weights, 1, 2)

    halo = lax.all_to_all(sends[0], "dom", 0, 0, tiled=True)
    h0, own = first_call(
        tile_columns, features, jnp.swapaxes(w_input, 0, 1), tile_values, steps
    )
    z = halo_call(
        tile_columns, [halo], tile_values, own_tiles, steps, n_dom, (own, h0)
    )
    pushed = [h0]
    for layer in range(layers):
        beta = math.log(LAMBDA_DECAY / (layer + 1) + 1.0)
        if layer + 1 < layers:
            z, send = lax.optimization_barrier((z, sends[layer + 1]))
            parts = feat_parts(z, n_feat)
            halos = [flip(send[k], "dom", n_dom, k) for k in range(1, n_dom)]
            halo_agg = halo_call(
                shift_columns, halos, tile_values, own_tiles, steps, n_dom
            )
            h, z = step_call(
                beta, tile_columns, parts, weights[layer], tile_values, halo_agg, h0, 2, steps
            )
            pushed.append(h)
        else:
            final = last_call(beta, feat_parts(z, n_feat), weights[layer], 2)
    return jnp.swapaxes(jnp.stack(pushed), 1, 2), jnp.swapaxes(final, 0, 1)


def solution(mesh):
    placed = (
        P("dom", None),
        P(None, "feat"),
        P(),
        P(None, "dom", "feat"),
        P("dom", None, None, None),
        P("dom", None),
        P("dom", None, None),
        P("dom", None),
    )
    return jax.shard_map(
        functools.partial(on_device, mesh.shape["feat"], mesh.shape["dom"]),
        mesh=mesh,
        in_specs=placed,
        out_specs=(P(None, "dom", "feat"), P("dom", "feat")),
        check_vma=False,
    )
```

```python
import functools
import math

import jax
import jax.numpy as jnp
from jax import lax
from jax.experimental import pallas as pl
from jax.experimental.pallas import tpu as pltpu
from jax.sharding import PartitionSpec as P

ALPHA = 0.1
LAMBDA_DECAY = 0.5
OWN_TILES_PER_ROW = 2
LANES = 128
NT = (((1,), (1,)), ((), ()))
F32 = jnp.float32
BF16 = jnp.bfloat16


def gather_kernel(rows_ref, counts_ref, hist_ref, out_ref, table, picked):
    layers, width, nodes = hist_ref.shape
    dest = pl.program_id(0)
    slots = picked.shape[0]

    @pl.when(dest == 0)
    def _():
        for start in range(0, nodes, 512):
            part = hist_ref[:, :, start : start + 512]
            table[start : start + 512, :] = part.reshape(layers * width, 512).astype(F32).T

    def step(block, carry):
        base = pl.multiple_of(block * 32, 32)
        for u in range(32):
            row = rows_ref[dest, base + u]
            picked[pl.ds(base + u, 1), :] = table[pl.ds(row, 1), :]
        return carry

    lax.fori_loop(0, slots // 32, step, 0)
    live = lax.broadcasted_iota(jnp.int32, (1, slots), 1) < counts_ref[0, dest]
    out_ref[0] = jnp.where(live, picked[...].T, 0.0).astype(BF16)


def gather_halo(send_rows, send_counts, hist, group, per_group):
    _, width, nodes = hist.shape
    peers, slots = send_rows.shape
    span = per_group * width
    return pl.pallas_call(
        gather_kernel,
        grid_spec=pltpu.PrefetchScalarGridSpec(
            num_scalar_prefetch=2,
            grid=(peers,),
            in_specs=[
                pl.BlockSpec((per_group, width, nodes), lambda k, rows, counts: (group, 0, 0))
            ],
            out_specs=pl.BlockSpec((1, span, slots), lambda k, rows, counts: (k, 0, 0)),
            scratch_shapes=[pltpu.VMEM((nodes, span), F32), pltpu.VMEM((slots, span), F32)],
        ),
        out_shape=jax.ShapeDtypeStruct((peers, span, slots), BF16),
        name="gather_halo",
    )(send_rows, send_counts, hist)


def tiles_dot(left_tiles, values):
    left = jnp.concatenate(left_tiles, axis=1)
    right = jnp.concatenate([values[k] for k in range(values.shape[0])], axis=1)
    return lax.dot_general(left, right, NT, preferred_element_type=F32)


def own_share(cols_ref, values_ref, state, first_row, row, tile):
    picks = []
    for k in range(OWN_TILES_PER_ROW):
        start = pl.multiple_of(cols_ref[first_row + row, k] * tile, tile)
        picks.append(state[:, pl.ds(start, tile)])
    return tiles_dot(picks, values_ref[row])


def blend(agg, initial):
    return ((1.0 - ALPHA) * agg + ALPHA * initial.astype(F32)).astype(BF16)


def first_kernel(steps, cols_ref, feat_ref, w_ref, values_ref, h_ref, loc_ref, state):
    i = pl.program_id(0)
    rows, _, tile, _ = values_ref.shape
    span = rows * tile

    @pl.when(i == 0)
    def _():
        prod = lax.dot_general(w_ref[...], feat_ref[...], NT, preferred_element_type=F32)
        h0 = jnp.maximum(prod, 0.0).astype(BF16)
        state[...] = h0
        h_ref[...] = h0

    for r in range(rows):
        loc_ref[:, r * tile : (r + 1) * tile] = own_share(
            cols_ref, values_ref, state, i * rows, r, tile
        )


def first_call(cols, features, w_t, values, steps):
    nodes = features.shape[0]
    width = w_t.shape[0]
    row_tiles, per_row, tile, _ = values.shape
    rows = row_tiles // steps
    whole = lambda shape: pl.BlockSpec(shape, lambda i, c: (0,) * len(shape))
    return pl.pallas_call(
        functools.partial(first_kernel, steps),
        grid_spec=pltpu.PrefetchScalarGridSpec(
            num_scalar_prefetch=1,
            grid=(steps,),
            in_specs=[
                whole(features.shape),
                whole(w_t.shape),
                pl.BlockSpec((rows, OWN_TILES_PER_ROW, tile, tile), lambda i, c: (i, 0, 0, 0)),
            ],
            out_specs=[
                whole((width, nodes)),
                pl.BlockSpec((width, rows * tile), lambda i, c: (0, i)),
            ],
            scratch_shapes=[pltpu.VMEM((width, nodes), BF16)],
        ),
        out_shape=[
            jax.ShapeDtypeStruct((width, nodes), BF16),
            jax.ShapeDtypeStruct((width, nodes), F32),
        ],
        name="first_own",
    )(cols, features, w_t, values)


def halo_kernel(n_values, blended, own_tiles, cols_ref, halo_ref, *refs):
    i = pl.program_id(0)
    values_refs, refs = refs[:n_values], refs[n_values:]
    rows, _, tile, _ = values_refs[0].shape
    per_peer = halo_ref.shape[2] // tile
    agg_ref = refs[-1]
    for r in range(rows):
        picks = []
        for k in range(OWN_TILES_PER_ROW, OWN_TILES_PER_ROW * (1 + n_values)):
            slot = cols_ref[i * rows + r, k] - own_tiles
            start = pl.multiple_of((slot % per_peer) * tile, tile)
            picks.append(halo_ref[slot // per_peer, :, pl.ds(start, tile)])
        values = jnp.concatenate([v[r] for v in values_refs], axis=0)
        agg = tiles_dot(picks, values)
        at = slice(r * tile, (r + 1) * tile)
        agg_ref[:, at] = agg
        if blended:
            own_ref, h0_ref, z_ref = refs[:3]
            width = z_ref.shape[0]
            z_ref[:, at] = blend(own_ref[:, at] + agg[:width], h0_ref[:, at])


def halo_call(cols, halo, values, own_tiles, steps, extra=()):
    row_tiles, per_row, tile, _ = values.shape
    rows = row_tiles // steps
    span = halo.shape[1]
    n_values = per_row // OWN_TILES_PER_ROW - 1
    column = lambda width: pl.BlockSpec((width, rows * tile), lambda i, c: (0, i))
    values_spec = lambda n: pl.BlockSpec(
        (rows, OWN_TILES_PER_ROW, tile, tile), lambda i, c: (i, n, 0, 0)
    )
    aggs = jax.ShapeDtypeStruct((span, row_tiles * tile), F32)
    outs, out_specs = [aggs], [column(span)]
    if extra:
        width = extra[1].shape[0]
        outs = [jax.ShapeDtypeStruct((width, row_tiles * tile), BF16)] + outs
        out_specs = [column(width)] + out_specs
    return pl.pallas_call(
        functools.partial(halo_kernel, n_values, bool(extra), own_tiles),
        grid_spec=pltpu.PrefetchScalarGridSpec(
            num_scalar_prefetch=1,
            grid=(steps,),
            in_specs=[pl.BlockSpec(halo.shape, lambda i, c: (0, 0, 0))]
            + [values_spec(n + 1) for n in range(n_values)]
            + [column(e.shape[0]) for e in extra],
            out_specs=out_specs,
        ),
        out_shape=outs,
        name="halo_share",
    )(cols, halo, *([values] * n_values), *extra)


def fresh_rows(beta, weight, parts):
    joined = jnp.concatenate(parts, axis=0)
    product = jnp.dot(weight, joined, preferred_element_type=F32)
    return jnp.maximum((1.0 - beta) * parts[0].astype(F32) + beta * product, 0.0).astype(BF16)


def step_kernel(beta, pieces, front, cols_ref, *refs):
    parts = refs[:pieces]
    w_ref, values_ref, halo_ref, h0_ref, h_ref, z_ref, state = refs[pieces:]
    i = pl.program_id(0)
    rows, _, tile, _ = values_ref.shape

    @pl.when(i < front)
    def _():
        fresh = fresh_rows(beta, w_ref[...], [p[...] for p in parts])
        span = fresh.shape[1]
        h_ref[...] = fresh
        state[:, pl.ds(pl.multiple_of(i * span, span), span)] = fresh

    @pl.when(i >= front)
    def _():
        for r in range(rows):
            agg = own_share(cols_ref, values_ref, state, (i - front) * rows, r, tile)
            at = slice(r * tile, (r + 1) * tile)
            z_ref[:, at] = blend(agg + halo_ref[:, at], h0_ref[:, at])


def step_call(beta, cols, parts, weight, values, halo_agg, place, h0, front, back):
    width, nodes = h0.shape
    row_tiles, per_row, tile, _ = values.shape
    rows = row_tiles // back
    early = lambda i, c: (0, jnp.minimum(i, front - 1))
    late = lambda i, c: (0, jnp.maximum(i - front, 0))
    late_block = pl.BlockSpec((width, rows * tile), late)
    return pl.pallas_call(
        functools.partial(step_kernel, beta, len(parts), front),
        grid_spec=pltpu.PrefetchScalarGridSpec(
            num_scalar_prefetch=1,
            grid=(front + back,),
            in_specs=[pl.BlockSpec((width, nodes // front), early) for _ in parts]
            + [
                pl.BlockSpec(weight.shape, lambda i, c: (0, 0)),
                pl.BlockSpec(
                    (rows, OWN_TILES_PER_ROW, tile, tile),
                    lambda i, c: (jnp.maximum(i - front, 0), 0, 0, 0),
                ),
                pl.BlockSpec(
                    (width, rows * tile),
                    lambda i, c: (place, jnp.maximum(i - front, 0)),
                ),
                late_block,
            ],
            out_specs=[pl.BlockSpec((width, nodes // front), early), late_block],
            scratch_shapes=[pltpu.VMEM((width, nodes), BF16)],
        ),
        out_shape=[jax.ShapeDtypeStruct((width, nodes), BF16)] * 2,
        name="layer_step",
    )(cols, *parts, weight, values, halo_agg, h0)


def last_kernel(beta, *refs):
    *parts, w_ref, h_ref = refs
    h_ref[...] = fresh_rows(beta, w_ref[...], [p[...] for p in parts])


def last_call(beta, parts, weight, steps):
    width, nodes = parts[0].shape
    column = pl.BlockSpec((width, nodes // steps), lambda i: (0, i))
    return pl.pallas_call(
        functools.partial(last_kernel, beta),
        grid=(steps,),
        in_specs=[column] * len(parts) + [pl.BlockSpec(weight.shape, lambda i: (0, 0))],
        out_specs=column,
        out_shape=jax.ShapeDtypeStruct((width, nodes), BF16),
        name="last_step",
    )(*parts, weight)


def flip(array, axis, size, shift):
    return lax.ppermute(array, axis, [(i, i ^ shift) for i in range(size)])


def feat_parts(z, n_feat):
    parts = [None] * n_feat
    parts[0] = z
    for shift in range(2, n_feat, 2):
        parts[shift] = flip(z, "feat", n_feat, shift)
    for shift in range(0, n_feat, 2):
        parts[shift + 1] = flip(parts[shift], "feat", n_feat, 1)
    return parts


def on_device(
    n_feat, features, w_input, layer_weights, history, tile_values, tile_columns,
    send_rows, send_counts,
):
    layers = history.shape[0]
    nodes = features.shape[0]
    width = w_input.shape[1]
    tile = tile_values.shape[-1]
    own_tiles = nodes // tile
    feat = lax.axis_index("feat")
    steps = 4

    hist = jnp.swapaxes(history, 1, 2)
    per_group = min(layers, LANES // width)
    sends = [
        gather_halo(send_rows[0], send_counts, hist, g, per_group)
        for g in range(layers // per_group)
    ]

    mine = lax.dynamic_slice_in_dim(layer_weights, feat * width, width, 2)
    weights = jnp.concatenate(
        [
            lax.dynamic_slice_in_dim(mine, (feat ^ shift) * width, width, 1)
            for shift in range(n_feat)
        ],
        axis=1,
    )
    weights = jnp.swapaxes(weights, 1, 2)

    halo = lax.all_to_all(sends[0], "dom", 0, 0, tiled=True)
    h0, own = first_call(
        tile_columns, features, jnp.swapaxes(w_input, 0, 1), tile_values, steps
    )
    z, aggs = halo_call(tile_columns, halo, tile_values, own_tiles, steps, (own, h0))
    aggs = [aggs]
    pushed = [h0]
    for layer in range(layers):
        beta = math.log(LAMBDA_DECAY / (layer + 1) + 1.0)
        if layer == 0:
            for send in sends[1:]:
                z, send = lax.optimization_barrier((z, send))
                halo = lax.all_to_all(send, "dom", 0, 0, tiled=True)
                aggs += halo_call(tile_columns, halo, tile_values, own_tiles, steps)
        parts = feat_parts(z, n_feat)
        if layer + 1 < layers:
            group, place = divmod(layer + 1, per_group)
            h, z = step_call(
                beta, tile_columns, parts, weights[layer], tile_values, aggs[group], place,
                h0, 2, steps,
            )
            pushed.append(h)
        else:
            final = last_call(beta, parts, weights[layer], 2)
    return jnp.swapaxes(jnp.stack(pushed), 1, 2), jnp.swapaxes(final, 0, 1)


def solution(mesh):
    placed = (
        P("dom", None),
        P(None, "feat"),
        P(),
        P(None, "dom", "feat"),
        P("dom", None, None, None),
        P("dom", None),
        P("dom", None, None),
        P("dom", None),
    )
    return jax.shard_map(
        functools.partial(on_device, mesh.shape["feat"]),
        mesh=mesh,
        in_specs=placed,
        out_specs=(P(None, "dom", "feat"), P("dom", "feat")),
        check_vma=False,
    )
```

```python
import functools
import math

import jax
import jax.numpy as jnp
from jax import lax
from jax.experimental import pallas as pl
from jax.experimental.pallas import tpu as pltpu
from jax.sharding import PartitionSpec as P

ALPHA = 0.1
LAMBDA_DECAY = 0.5
OWN_TILES_PER_ROW = 2
LANES = 128
NT = (((1,), (1,)), ((), ()))
F32 = jnp.float32
BF16 = jnp.bfloat16


def gather_kernel(rows_ref, counts_ref, hist_ref, out_ref, table, picked):
    layers, width, nodes = hist_ref.shape
    dest = pl.program_id(0)
    slots = picked.shape[0]

    @pl.when(dest == 0)
    def _():
        for start in range(0, nodes, 512):
            part = hist_ref[:, :, start : start + 512]
            table[start : start + 512, :] = part.reshape(layers * width, 512).astype(F32).T

    def step(block, carry):
        base = pl.multiple_of(block * 32, 32)
        ids = [rows_ref[dest, base + u] for u in range(32)]
        loaded = [table[pl.ds(row, 1), :] for row in ids]
        for u in range(32):
            picked[pl.ds(base + u, 1), :] = loaded[u]
        return carry

    lax.fori_loop(0, slots // 32, step, 0)
    live = lax.broadcasted_iota(jnp.int32, (1, slots), 1) < counts_ref[0, dest]
    out_ref[0] = jnp.where(live, picked[...].T, 0.0).astype(BF16)


def gather_halo(send_rows, send_counts, hist, group, per_group):
    _, width, nodes = hist.shape
    peers, slots = send_rows.shape
    span = per_group * width
    return pl.pallas_call(
        gather_kernel,
        grid_spec=pltpu.PrefetchScalarGridSpec(
            num_scalar_prefetch=2,
            grid=(peers,),
            in_specs=[
                pl.BlockSpec((per_group, width, nodes), lambda k, rows, counts: (group, 0, 0))
            ],
            out_specs=pl.BlockSpec((1, span, slots), lambda k, rows, counts: (k, 0, 0)),
            scratch_shapes=[pltpu.VMEM((nodes, span), F32), pltpu.VMEM((slots, span), F32)],
        ),
        out_shape=jax.ShapeDtypeStruct((peers, span, slots), BF16),
        name="gather_halo",
    )(send_rows, send_counts, hist)


def tiles_dot(left_tiles, values):
    left = jnp.concatenate(left_tiles, axis=1)
    right = jnp.concatenate([values[k] for k in range(values.shape[0])], axis=1)
    return lax.dot_general(left, right, NT, preferred_element_type=F32)


def own_share(cols_ref, values_ref, state, first_row, row, tile):
    picks = []
    for k in range(OWN_TILES_PER_ROW):
        start = pl.multiple_of(cols_ref[first_row + row, k] * tile, tile)
        picks.append(state[:, pl.ds(start, tile)])
    return tiles_dot(picks, values_ref[row])


def blend(agg, initial):
    return ((1.0 - ALPHA) * agg + ALPHA * initial.astype(F32)).astype(BF16)


def first_kernel(steps, cols_ref, feat_ref, w_ref, values_ref, h_ref, loc_ref, state):
    i = pl.program_id(0)
    rows, _, tile, _ = values_ref.shape
    span = rows * tile

    @pl.when(i == 0)
    def _():
        prod = lax.dot_general(w_ref[...], feat_ref[...], NT, preferred_element_type=F32)
        h0 = jnp.maximum(prod, 0.0).astype(BF16)
        state[...] = h0
        h_ref[...] = h0

    for r in range(rows):
        loc_ref[:, r * tile : (r + 1) * tile] = own_share(
            cols_ref, values_ref, state, i * rows, r, tile
        )


def first_call(cols, features, w_t, values, steps):
    nodes = features.shape[0]
    width = w_t.shape[0]
    row_tiles, per_row, tile, _ = values.shape
    rows = row_tiles // steps
    whole = lambda shape: pl.BlockSpec(shape, lambda i, c: (0,) * len(shape))
    return pl.pallas_call(
        functools.partial(first_kernel, steps),
        grid_spec=pltpu.PrefetchScalarGridSpec(
            num_scalar_prefetch=1,
            grid=(steps,),
            in_specs=[
                whole(features.shape),
                whole(w_t.shape),
                pl.BlockSpec((rows, OWN_TILES_PER_ROW, tile, tile), lambda i, c: (i, 0, 0, 0)),
            ],
            out_specs=[
                whole((width, nodes)),
                pl.BlockSpec((width, rows * tile), lambda i, c: (0, i)),
            ],
            scratch_shapes=[pltpu.VMEM((width, nodes), BF16)],
        ),
        out_shape=[
            jax.ShapeDtypeStruct((width, nodes), BF16),
            jax.ShapeDtypeStruct((width, nodes), F32),
        ],
        name="first_own",
    )(cols, features, w_t, values)


def halo_kernel(n_values, blended, own_tiles, cols_ref, halo_ref, *refs):
    i = pl.program_id(0)
    values_refs, refs = refs[:n_values], refs[n_values:]
    rows, _, tile, _ = values_refs[0].shape
    per_peer = halo_ref.shape[2] // tile
    agg_ref = refs[-1]
    for r in range(rows):
        picks = []
        for k in range(OWN_TILES_PER_ROW, OWN_TILES_PER_ROW * (1 + n_values)):
            slot = cols_ref[i * rows + r, k] - own_tiles
            start = pl.multiple_of((slot % per_peer) * tile, tile)
            picks.append(halo_ref[slot // per_peer, :, pl.ds(start, tile)])
        values = jnp.concatenate([v[r] for v in values_refs], axis=0)
        agg = tiles_dot(picks, values)
        at = slice(r * tile, (r + 1) * tile)
        agg_ref[:, at] = agg
        if blended:
            own_ref, h0_ref, z_ref = refs[:3]
            width = z_ref.shape[0]
            z_ref[:, at] = blend(own_ref[:, at] + agg[:width], h0_ref[:, at])


def halo_call(cols, halo, values, own_tiles, steps, extra=()):
    row_tiles, per_row, tile, _ = values.shape
    rows = row_tiles // steps
    span = halo.shape[1]
    n_values = per_row // OWN_TILES_PER_ROW - 1
    column = lambda width: pl.BlockSpec((width, rows * tile), lambda i, c: (0, i))
    values_spec = lambda n: pl.BlockSpec(
        (rows, OWN_TILES_PER_ROW, tile, tile), lambda i, c: (i, n, 0, 0)
    )
    aggs = jax.ShapeDtypeStruct((span, row_tiles * tile), F32)
    outs, out_specs = [aggs], [column(span)]
    if extra:
        width = extra[1].shape[0]
        outs = [jax.ShapeDtypeStruct((width, row_tiles * tile), BF16)] + outs
        out_specs = [column(width)] + out_specs
    return pl.pallas_call(
        functools.partial(halo_kernel, n_values, bool(extra), own_tiles),
        grid_spec=pltpu.PrefetchScalarGridSpec(
            num_scalar_prefetch=1,
            grid=(steps,),
            in_specs=[pl.BlockSpec(halo.shape, lambda i, c: (0, 0, 0))]
            + [values_spec(n + 1) for n in range(n_values)]
            + [column(e.shape[0]) for e in extra],
            out_specs=out_specs,
        ),
        out_shape=outs,
        name="halo_share",
    )(cols, halo, *([values] * n_values), *extra)


def fresh_rows(beta, weight, parts):
    joined = jnp.concatenate(parts, axis=0)
    product = jnp.dot(weight, joined, preferred_element_type=F32)
    return jnp.maximum((1.0 - beta) * parts[0].astype(F32) + beta * product, 0.0).astype(BF16)


def step_kernel(beta, pieces, front, cols_ref, *refs):
    parts = refs[:pieces]
    w_ref, values_ref, halo_ref, h0_ref, h_ref, z_ref, state = refs[pieces:]
    i = pl.program_id(0)
    rows, _, tile, _ = values_ref.shape

    @pl.when(i < front)
    def _():
        fresh = fresh_rows(beta, w_ref[...], [p[...] for p in parts])
        span = fresh.shape[1]
        h_ref[...] = fresh
        state[:, pl.ds(pl.multiple_of(i * span, span), span)] = fresh

    @pl.when(i >= front)
    def _():
        for r in range(rows):
            agg = own_share(cols_ref, values_ref, state, (i - front) * rows, r, tile)
            at = slice(r * tile, (r + 1) * tile)
            z_ref[:, at] = blend(agg + halo_ref[:, at], h0_ref[:, at])


def step_call(beta, cols, parts, weight, values, halo_agg, place, h0, front, back):
    width, nodes = h0.shape
    row_tiles, per_row, tile, _ = values.shape
    rows = row_tiles // back
    early = lambda i, c: (0, jnp.minimum(i, front - 1))
    late = lambda i, c: (0, jnp.maximum(i - front, 0))
    late_block = pl.BlockSpec((width, rows * tile), late)
    return pl.pallas_call(
        functools.partial(step_kernel, beta, len(parts), front),
        grid_spec=pltpu.PrefetchScalarGridSpec(
            num_scalar_prefetch=1,
            grid=(front + back,),
            in_specs=[pl.BlockSpec((width, nodes // front), early) for _ in parts]
            + [
                pl.BlockSpec(weight.shape, lambda i, c: (0, 0)),
                pl.BlockSpec(
                    (rows, OWN_TILES_PER_ROW, tile, tile),
                    lambda i, c: (jnp.maximum(i - front, 0), 0, 0, 0),
                ),
                pl.BlockSpec(
                    (width, rows * tile),
                    lambda i, c: (place, jnp.maximum(i - front, 0)),
                ),
                late_block,
            ],
            out_specs=[pl.BlockSpec((width, nodes // front), early), late_block],
            scratch_shapes=[pltpu.VMEM((width, nodes), BF16)],
        ),
        out_shape=[jax.ShapeDtypeStruct((width, nodes), BF16)] * 2,
        name="layer_step",
    )(cols, *parts, weight, values, halo_agg, h0)


def last_kernel(beta, *refs):
    *parts, w_ref, h_ref = refs
    h_ref[...] = fresh_rows(beta, w_ref[...], [p[...] for p in parts])


def last_call(beta, parts, weight, steps):
    width, nodes = parts[0].shape
    column = pl.BlockSpec((width, nodes // steps), lambda i: (0, i))
    return pl.pallas_call(
        functools.partial(last_kernel, beta),
        grid=(steps,),
        in_specs=[column] * len(parts) + [pl.BlockSpec(weight.shape, lambda i: (0, 0))],
        out_specs=column,
        out_shape=jax.ShapeDtypeStruct((width, nodes), BF16),
        name="last_step",
    )(*parts, weight)


def flip(array, axis, size, shift):
    return lax.ppermute(array, axis, [(i, i ^ shift) for i in range(size)])


def feat_parts(z, n_feat, covered):
    parts = [None] * n_feat
    parts[0] = z
    parts[1] = flip(z, "feat", n_feat, 1)
    far = [flip(z, "feat", n_feat, shift) for shift in range(2, n_feat, 2)]
    if covered is not None:
        far, covered = lax.optimization_barrier((far, covered))
    for place, array in enumerate(far):
        parts[2 * place + 2] = array
        parts[2 * place + 3] = flip(array, "feat", n_feat, 1)
    return parts, covered


def on_device(
    n_feat, features, w_input, layer_weights, history, tile_values, tile_columns,
    send_rows, send_counts,
):
    layers = history.shape[0]
    nodes = features.shape[0]
    width = w_input.shape[1]
    tile = tile_values.shape[-1]
    own_tiles = nodes // tile
    feat = lax.axis_index("feat")
    steps = 4

    hist = jnp.swapaxes(history, 1, 2)
    per_group = min(layers, LANES // width)
    sends = [
        gather_halo(send_rows[0], send_counts, hist, g, per_group)
        for g in range(layers // per_group)
    ]

    mine = lax.dynamic_slice_in_dim(layer_weights, feat * width, width, 2)
    weights = jnp.concatenate(
        [
            lax.dynamic_slice_in_dim(mine, (feat ^ shift) * width, width, 1)
            for shift in range(n_feat)
        ],
        axis=1,
    )
    weights = jnp.swapaxes(weights, 1, 2)

    halo = lax.all_to_all(sends[0], "dom", 0, 0, tiled=True)
    h0, own = first_call(
        tile_columns, features, jnp.swapaxes(w_input, 0, 1), tile_values, steps
    )
    weights = [weights[i] for i in range(layers)]
    halo, own, weights, sends[1:] = lax.optimization_barrier((halo, own, weights, sends[1:]))
    halos = [lax.all_to_all(send, "dom", 0, 0, tiled=True) for send in sends[1:]]
    z, aggs = halo_call(tile_columns, halo, tile_values, own_tiles, steps, (own, h0))
    aggs = [aggs]
    pushed = [h0]
    for layer in range(layers):
        beta = math.log(LAMBDA_DECAY / (layer + 1) + 1.0)
        if layer == 0:
            for later in halos:
                aggs += halo_call(tile_columns, later, tile_values, own_tiles, steps)
            parts, _ = feat_parts(z, n_feat, None)
        elif layer == per_group - 1 and layer < layers - 1:
            parts, aggs[1:] = feat_parts(z, n_feat, aggs[1:])
        elif layer == layers - 1:
            parts, stacked = feat_parts(z, n_feat, jnp.stack(pushed))
        else:
            parts, _ = feat_parts(z, n_feat, None)
        if layer + 1 < layers:
            group, place = divmod(layer + 1, per_group)
            h, z = step_call(
                beta, tile_columns, parts, weights[layer], tile_values, aggs[group], place,
                h0, 2, steps,
            )
            pushed.append(h)
        else:
            final = last_call(beta, parts, weights[layer], 2)
    return jnp.swapaxes(stacked, 1, 2), jnp.swapaxes(final, 0, 1)


def solution(mesh):
    placed = (
        P("dom", None),
        P(None, "feat"),
        P(),
        P(None, "dom", "feat"),
        P("dom", None, None, None),
        P("dom", None),
        P("dom", None, None),
        P("dom", None),
    )
    return jax.shard_map(
        functools.partial(on_device, mesh.shape["feat"]),
        mesh=mesh,
        in_specs=placed,
        out_specs=(P(None, "dom", "feat"), P("dom", "feat")),
        check_vma=False,
    )
```
